32 devices in a mesh: rep: 2 (over y), gx: 4 (over x, core), gy: 4 (over z).
Axes of the slice: x: 2, y: 2, z: 4, core: 2. Of those that a mesh axis runs over, the one named last changes fastest.
Arguments:
- deltas: bfloat16 [2, 2, 3584, 14336], P('rep', None, 'gx', 'gy'), may hold values from -32 to 32
- params: float32 [2, 4, 4, 2, 4, 4, 112, 896], P(None, None, 'gx', 'rep', None, 'gy'), may hold values from -0.75 to 0.75
- momentum: float32 [2, 4, 4, 2, 4, 4, 112, 896], P(None, None, 'gx', 'rep', None, 'gy'), may hold values from -1.5 to 1.5
Outputs:
- new_params: float32 [2, 4, 4, 2, 4, 4, 112, 896], P(None, None, 'gx', 'rep', None, 'gy')
- new_momentum: float32 [2, 4, 4, 2, 4, 4, 112, 896], P(None, None, 'gx', 'rep', None, 'gy')
The draws below stay inside these ranges and needn't reach their ends.
All inputs are finite; a program needn't handle non-finite values.
Results may differ from the reference program's by a relative error of at most 0.0003.
Values may be sent and summed in bfloat16 or wider, within the bound.
A program may use at most 128 MiB of HBM per device.

```python
import math
import jax
import jax.numpy as jnp
from jax import lax

D = 3584
FF = 14336
REPLICAS = 2
ROW_SPLIT = 4
COL_SPLIT = 4
ROW_TILE = 112
COL_TILE = 896


def draw_deltas(key, part):
    row_key, col_key, own_key = jax.random.split(key, 3)
    devices_all = REPLICAS * ROW_SPLIT * COL_SPLIT
    divisor = 2.0 * max(devices_all - 1, 1)
    rows_at = jnp.arange(D) % (D // ROW_SPLIT) // ROW_TILE
    rep_at = rows_at % REPLICAS
    gx_at = rows_at // REPLICAS
    cols_at = jnp.arange(FF) % (FF // COL_SPLIT) // COL_TILE
    row_ramp = jnp.exp(math.log(3.0) * (rep_at * ROW_SPLIT * COL_SPLIT + gx_at * COL_SPLIT).astype(jnp.float32) / divisor)
    col_ramp = jnp.exp(math.log(3.0) * cols_at.astype(jnp.float32) / divisor)
    row_scale = jnp.power(10.0, jax.random.uniform(row_key, (2, D, 1), jnp.float32)) * row_ramp[None, :, None]
    col_scale = jnp.power(10.0, jax.random.uniform(col_key, (2, 1, FF), jnp.float32)) * col_ramp[None, None, :]
    spread = 0.1 * row_scale * col_scale

    def draw_replica(replica):
        sample = jax.random.truncated_normal(jax.random.fold_in(own_key, replica), -6.0, 6.0, (2, D, FF), jnp.float32)
        value = jnp.clip(sample * spread, -32.0, 32.0)
        return value.astype(jnp.bfloat16)
    return lax.map(draw_replica, jnp.arange(REPLICAS))


def shard_levels(key, extent, pieces, low, top_value):
    def one(position, blocks):
        heights = jax.random.uniform(jax.random.fold_in(jax.random.fold_in(key, 6), position), (blocks,), jnp.float32, low / len(pieces), top_value / len(pieces))
        return jnp.repeat(jnp.exp(heights), extent[position] // blocks).reshape((-1,) + (1,) * (len(extent) - position - 1))

    loudness = one(*pieces[0])
    for cut in pieces[1:]:
        loudness = loudness * one(*cut)
    return loudness


def bell_draw(key, shape, width, reach, shards=(), kind=jnp.bfloat16):
    values = jax.random.normal(key, shape, jnp.float32) * width
    if len(shards) > 0:
        values = shard_levels(key, shape, shards, -0.22, 0.18) * values
    return jnp.clip(values, min=-reach, max=reach).astype(kind)


def setup_inputs(seed: int = 0) -> dict:
    seeds = jax.random.split(jax.random.key(seed), 4)
    return {
        "deltas": draw_deltas(jax.random.fold_in(seeds[3], 71), 0),
        "params": bell_draw(seeds[1], (2, ROW_SPLIT, ROW_SPLIT, REPLICAS, COL_SPLIT, COL_SPLIT, ROW_TILE, COL_TILE), 0.05, 0.75, ((2, 4), (3, 2), (5, 4)), jnp.float32),
        "momentum": bell_draw(seeds[2], (2, ROW_SPLIT, ROW_SPLIT, REPLICAS, COL_SPLIT, COL_SPLIT, ROW_TILE, COL_TILE), 0.1, 1.5, ((2, 4), (3, 2), (5, 4)), jnp.float32),
    }


clip_level = 0.25
moment_decay = 0.9
outer_rate = 0.7
epsilon = 1e-06

def reference(deltas, params, momentum):
    running = jnp.zeros(deltas.shape[1:], jnp.float32)
    for replica in range(REPLICAS):
        running = running + deltas[replica].astype(jnp.float32)
    mean_delta = running / REPLICAS
    squares = jnp.sum(mean_delta * mean_delta)
    entries = mean_delta.size
    root_mean = jnp.sqrt(squares / entries + epsilon)
    clip_scale = jnp.minimum(1.0, clip_level / root_mean)
    blocked = mean_delta.reshape(2, ROW_SPLIT, ROW_SPLIT, REPLICAS, ROW_TILE, COL_SPLIT, COL_SPLIT, COL_TILE)
    blocked = jnp.transpose(blocked, (0, 1, 2, 3, 5, 6, 4, 7))
    gradient = clip_scale * blocked
    new_momentum = moment_decay * momentum + gradient
    new_params = params - outer_rate * (gradient + moment_decay * new_momentum)
    return (new_params, new_momentum)
```

```python
import functools

import jax
import jax.numpy as jnp
from jax import lax
from jax.experimental import pallas as pl
from jax.experimental.pallas import tpu as pltpu
from jax.sharding import PartitionSpec as P

clip_level = 0.25
moment_decay = 0.9
outer_rate = 0.7
epsilon = 1e-06

MESH = pl.DeviceIdType.MESH
LANES = 128
TOP = 240.0
SMALLEST = 1e-30
SLOTS = 4
PREFETCH_AT = 2
EXCHANGE_VMEM = 22 * 1024 * 1024
UPDATE_VMEM = 14 * 1024 * 1024


def encode(value):
    power = value * value
    for _ in range(3):
        power = power * power
    return jnp.where(value < 0.0, -power, power).astype(jnp.bfloat16)


def decode(code):
    wide = code.astype(jnp.float32)
    root = jnp.exp2(jnp.log2(jnp.abs(wide)) * (1.0 / 16.0))
    root = jnp.where(wide == 0.0, 0.0, root)
    return jnp.where(wide < 0.0, -root, root)


def fold_lanes(tile, combine):
    folded = tile[:, :LANES]
    for start in range(LANES, tile.shape[1], LANES):
        folded = combine(folded, tile[:, start : start + LANES])
    return folded


def exchange(
    replicas, rows_split, cols_split, matrices,
    delta_ref, params_ref, momentum_ref, state_ref,
    own, peer, landed, peaks, landed_peaks, wide, total, mine, from_rep, middle, from_grid,
    own_sem, rep_send, rep_recv, tile_send, tile_recv, peak_send, peak_recv,
    first_send, first_recv, second_send, second_recv, state_sem,
):
    rep, gx, gy = lax.axis_index("rep"), lax.axis_index("gx"), lax.axis_index("gy")
    steps, rows, cols = own.shape
    grid = rows_split * cols_split
    far = rows_split * (cols_split - 1)
    far_steps = far * matrices
    remote_steps = steps - matrices
    band = total.shape[0]
    spread = max(cols_split - 1, 1)

    def place(step, sign):
        turn, matrix = step // matrices, step % matrices
        is_far = turn < far
        row_shift = jnp.where(is_far, turn // spread, (turn - far + 1) % rows_split)
        col_shift = jnp.where(is_far, 1 + (turn % spread + 1) % spread, 0)
        c = (gx + rows_split + sign * row_shift) % rows_split
        d = (gy + cols_split + sign * col_shift) % cols_split
        return matrix, c, d

    def block(step, replica):
        matrix, c, d = place(step, 1)
        return delta_ref.at[matrix, c, replica, :, pl.ds(pl.multiple_of(d * cols, LANES), cols)]

    def own_copy(step):
        return pltpu.make_async_copy(block(step, rep), own.at[step], own_sem.at[step])

    def rep_copy(shift, step):
        target = (rep + shift) % replicas
        return pltpu.make_async_remote_copy(
            src_ref=block(step, target), dst_ref=peer.at[shift - 1, step],
            send_sem=rep_send.at[shift - 1, step], recv_sem=rep_recv.at[shift - 1, step],
            device_id={"rep": target}, device_id_type=MESH,
        )

    def tile_copies(step):
        matrix, c, d = place(step, 1)
        target = {"gx": c, "gy": d}
        return (
            pltpu.make_async_remote_copy(
                src_ref=own.at[step], dst_ref=landed.at[step],
                send_sem=tile_send.at[step], recv_sem=tile_recv.at[step],
                device_id=target, device_id_type=MESH,
            ),
            pltpu.make_async_remote_copy(
                src_ref=peaks.at[step], dst_ref=landed_peaks.at[step],
                send_sem=peak_send.at[step], recv_sem=peak_recv.at[step],
                device_id=target, device_id_type=MESH,
            ),
        )

    def neighbour(shift):
        return (gx + shift // cols_split) % rows_split, (gy + shift % cols_split) % cols_split

    def state_copies():
        return (
            pltpu.make_async_copy(params_ref, state_ref.at[pl.ds(steps, steps)], state_sem.at[0]),
            pltpu.make_async_copy(momentum_ref, state_ref.at[pl.ds(2 * steps, steps)], state_sem.at[1]),
        )

    barrier = pltpu.get_barrier_semaphore()
    for shift in range(1, replicas):
        pl.semaphore_signal(
            barrier, inc=1, device_id={"rep": (rep + shift) % replicas}, device_id_type=MESH
        )

    def greet(shift, carry):
        c, d = neighbour(shift)
        pl.semaphore_signal(barrier, inc=1, device_id={"gx": c, "gy": d}, device_id_type=MESH)
        return carry

    lax.fori_loop(1, grid, greet, 0)
    pl.semaphore_wait(barrier, replicas - 1 + grid - 1)

    def launch(step, carry):
        own_copy(step).start()
        for shift in range(1, replicas):
            rep_copy(shift, step).start()
        return carry

    lax.fori_loop(0, steps, launch, 0)
    total[...] = jnp.zeros_like(total)

    def spot(matrix, c, d):
        return (matrix * rows_split + c) * cols_split + d

    def band_at(index):
        return pl.ds(pl.multiple_of(index * band, band), band)

    def mean_of(step, at):
        value = own[step, at, :].astype(jnp.float32)
        for shift in range(1, replicas):
            value = value + peer[shift - 1, step, at, :].astype(jnp.float32)
        value = value * (1.0 / replicas)
        total[...] += value * value
        return value

    def arrive(step):
        own_copy(step).wait()
        for shift in range(1, replicas):
            rep_copy(shift, step).wait_recv()

    def unpack(step):
        for copy in tile_copies(step):
            copy.wait_recv()
        matrix, c, d = place(step, -1)
        lift = jnp.concatenate([landed_peaks[step]] * (cols // LANES), axis=1)

        def part(index, carry):
            at = band_at(index)
            state_ref[spot(matrix, c, d), at, :] = decode(landed[step, at, :]) * lift
            return carry

        lax.fori_loop(0, rows // band, part, 0)

    def ready(step):
        return jnp.clip((3 * step - 8) // 4, 0, far_steps)

    def advance(step, carry):
        arrive(step)

        def average(index, peak):
            at = band_at(index)
            value = mean_of(step, at)
            wide[at, :] = value
            return jnp.maximum(peak, fold_lanes(jnp.abs(value), jnp.maximum))

        peak = lax.fori_loop(0, rows // band, average, jnp.zeros((band, LANES), jnp.float32))
        peak = jnp.maximum(jnp.max(peak, axis=0, keepdims=True), SMALLEST)
        peaks[step] = peak * (1.0 / TOP)
        lift = jnp.concatenate([TOP / peak] * (cols // LANES), axis=1)

        def code(index, carry):
            at = band_at(index)
            own[step, at, :] = encode(wide[at, :] * lift)
            return carry

        lax.fori_loop(0, rows // band, code, 0)
        for copy in tile_copies(step):
            copy.start()

        @pl.when(step == PREFETCH_AT)
        def _():
            for copy in state_copies():
                copy.start()

        @pl.when(ready(step) > ready(step - 1))
        def _():
            unpack(ready(step) - 1)

        @pl.when(step >= far_steps + 3)
        def _():
            unpack(step - 3)

        return carry

    lax.fori_loop(0, remote_steps, advance, 0)

    def keep(step, carry):
        arrive(step)
        matrix = step - remote_steps

        def average(index, inner):
            at = band_at(index)
            state_ref[spot(matrix, gx, gy), at, :] = mean_of(step, at)
            return inner

        return lax.fori_loop(0, rows // band, average, carry)

    lax.fori_loop(remote_steps, steps, keep, 0)

    mine[...] = jnp.sum(fold_lanes(total[...], jnp.add), axis=0, keepdims=True)

    def first_copy(shift):
        return pltpu.make_async_remote_copy(
            src_ref=mine, dst_ref=from_rep.at[shift - 1],
            send_sem=first_send.at[shift - 1], recv_sem=first_recv.at[shift - 1],
            device_id={"rep": (rep + shift) % replicas}, device_id_type=MESH,
        )

    def second_copy(shift):
        c, d = neighbour(shift)
        return pltpu.make_async_remote_copy(
            src_ref=middle, dst_ref=from_grid.at[shift - 1],
            send_sem=second_send.at[shift - 1], recv_sem=second_recv.at[shift - 1],
            device_id={"gx": c, "gy": d}, device_id_type=MESH,
        )

    for shift in range(1, replicas):
        first_copy(shift).start()
    subtotal = mine[...]
    for shift in range(1, replicas):
        first_copy(shift).wait()
        subtotal = subtotal + from_rep[shift - 1]
    middle[...] = subtotal
    lax.fori_loop(1, grid, lambda shift, carry: (second_copy(shift).start(), carry)[1], 0)

    last = ready(remote_steps - 1)
    lax.fori_loop(last, far_steps, lambda step, carry: (unpack(step), carry)[1], 0)
    lax.fori_loop(
        max(remote_steps - 3, far_steps), remote_steps, lambda step, carry: (unpack(step), carry)[1], 0
    )
    for copy in state_copies():
        copy.wait()

    def close_rep(step, carry):
        for shift in range(1, replicas):
            rep_copy(shift, step).wait_send()
        return carry

    lax.fori_loop(0, steps, close_rep, 0)

    def close_send(step, carry):
        for copy in tile_copies(step):
            copy.wait_send()
        return carry

    lax.fori_loop(0, remote_steps, close_send, 0)

    def gather(shift, carry):
        second_copy(shift).wait()
        return carry + from_grid[shift - 1]

    state_ref[3 * steps, :1, :LANES] = lax.fori_loop(1, grid, gather, subtotal)


def update(entries, state_ref, new_params_ref, new_momentum_ref, params_out, momentum_out, sems):
    count, (rows, cols) = state_ref.shape[0] // 3, state_ref.shape[1:]
    squares = jnp.sum(state_ref[3 * count, :1, :LANES], axis=1, keepdims=True)
    clip_scale = jnp.minimum(1.0, clip_level / jnp.sqrt(squares / entries + epsilon))
    band = 8 if rows % 8 == 0 else rows

    def copies(tile):
        slot = tile % SLOTS
        return (
            pltpu.make_async_copy(params_out.at[slot], new_params_ref.at[tile], sems.at[0, slot]),
            pltpu.make_async_copy(momentum_out.at[slot], new_momentum_ref.at[tile], sems.at[1, slot]),
        )

    def one(tile, carry):
        slot = tile % SLOTS

        @pl.when(tile >= SLOTS)
        def _():
            for copy in copies(tile - SLOTS):
                copy.wait()

        def part(index, inner):
            at = pl.ds(pl.multiple_of(index * band, band), band)
            gradient = state_ref[tile, at, :] * clip_scale
            new_momentum = moment_decay * state_ref[2 * count + tile, at, :] + gradient
            momentum_out[slot, at, :] = new_momentum
            params_out[slot, at, :] = state_ref[count + tile, at, :] - outer_rate * (
                gradient + moment_decay * new_momentum
            )
            return inner

        lax.fori_loop(0, rows // band, part, 0, unroll=2 if (rows // band) % 2 == 0 else 1)
        for copy in copies(tile):
            copy.start()
        return carry

    lax.fori_loop(0, count, one, 0)

    def close(tile, carry):
        for copy in copies(tile):
            copy.wait()
        return carry

    lax.fori_loop(max(count - SLOTS, 0), count, close, 0)


def per_device(deltas, params, momentum):
    rows_split = lax.axis_size("gx")
    cols_split = lax.axis_size("gy")
    replicas = lax.axis_size("rep")
    matrices, local_rows, local_cols = deltas.shape[1:]
    rows = local_rows // (rows_split * replicas)
    cols = local_cols // cols_split
    entries = matrices * local_rows * local_cols * rows_split * cols_split
    grid = rows_split * cols_split
    steps = grid * matrices
    band = 16 if rows % 16 == 0 else rows
    any_space = pl.BlockSpec(memory_space=pl.ANY)
    vmem = pl.BlockSpec(memory_space=pltpu.VMEM)
    dma = pltpu.SemaphoreType.DMA
    f32, bf16 = jnp.float32, jnp.bfloat16
    flat_shape = (steps, rows, cols)
    state = pl.pallas_call(
        functools.partial(exchange, replicas, rows_split, cols_split, matrices),
        out_shape=pltpu.VMEM((3 * steps + 1, rows, cols), f32),
        in_specs=[any_space] * 3,
        out_specs=vmem,
        scratch_shapes=[
            pltpu.VMEM(flat_shape, bf16),
            pltpu.VMEM((max(replicas - 1, 1), *flat_shape), bf16),
            pltpu.VMEM(flat_shape, bf16),
            pltpu.VMEM((steps, 1, LANES), f32),
            pltpu.VMEM((steps, 1, LANES), f32),
            pltpu.VMEM((rows, cols), f32),
            pltpu.VMEM((band, cols), f32),
            pltpu.VMEM((1, LANES), f32),
            pltpu.VMEM((max(replicas - 1, 1), 1, LANES), f32),
            pltpu.VMEM((1, LANES), f32),
            pltpu.VMEM((grid, 1, LANES), f32),
            dma((steps,)),
            dma((max(replicas - 1, 1), steps)),
            dma((max(replicas - 1, 1), steps)),
            dma((steps,)),
            dma((steps,)),
            dma((steps,)),
            dma((steps,)),
            dma((max(replicas - 1, 1),)),
            dma((max(replicas - 1, 1),)),
            dma((grid,)),
            dma((grid,)),
            dma((2,)),
        ],
        compiler_params=pltpu.CompilerParams(
            collective_id=0, has_side_effects=True, vmem_limit_bytes=EXCHANGE_VMEM
        ),
    )(
        deltas.reshape(matrices, rows_split, replicas, rows, local_cols),
        params.reshape(flat_shape),
        momentum.reshape(flat_shape),
    )
    wide_shape = jax.ShapeDtypeStruct(flat_shape, f32)
    new_params, new_momentum = pl.pallas_call(
        functools.partial(update, entries),
        out_shape=(wide_shape, wide_shape),
        in_specs=[vmem],
        out_specs=(any_space, any_space),
        scratch_shapes=[
            pltpu.VMEM((SLOTS, rows, cols), f32),
            pltpu.VMEM((SLOTS, rows, cols), f32),
            dma((2, SLOTS)),
        ],
        compiler_params=pltpu.CompilerParams(vmem_limit_bytes=UPDATE_VMEM),
    )(pltpu.with_memory_space_constraint(state, pltpu.VMEM))
    return (new_params.reshape(params.shape), new_momentum.reshape(momentum.shape))


def solution(mesh):
    placement = P(None, None, "gx", "rep", None, "gy", None, None)
    return jax.shard_map(
        per_device,
        mesh=mesh,
        in_specs=(P("rep", None, "gx", "gy"), placement, placement),
        out_specs=(placement, placement),
        check_vma=False,
    )
```

```python
import functools

import jax
import jax.numpy as jnp
from jax import lax
from jax.experimental import pallas as pl
from jax.experimental.pallas import tpu as pltpu
from jax.sharding import PartitionSpec as P

clip_level = 0.25
moment_decay = 0.9
outer_rate = 0.7
epsilon = 1e-06

MESH = pl.DeviceIdType.MESH
LANES = 128
TOP = 240.0
SMALLEST = 1e-30
SLOTS = 12
PREFETCH_AT = 4
READY_LAG = 21
NEAR_LAG = 5
EXCHANGE_VMEM = 22 * 1024 * 1024
UPDATE_VMEM = 20 * 1024 * 1024


def encode(value):
    power = value * value
    for _ in range(3):
        power = power * power
    return jnp.where(value < 0.0, -power, power).astype(jnp.bfloat16)


def decode(code):
    wide = code.astype(jnp.float32)
    root = jnp.exp2(jnp.log2(jnp.abs(wide)) * (1.0 / 16.0))
    root = jnp.where(wide == 0.0, 0.0, root)
    return jnp.where(wide < 0.0, -root, root)


def fold_lanes(tile, combine):
    folded = tile[:, :LANES]
    for start in range(LANES, tile.shape[1], LANES):
        folded = combine(folded, tile[:, start : start + LANES])
    return folded


def exchange(
    replicas, rows_split, cols_split, matrices,
    delta_ref, params_ref, momentum_ref, state_ref,
    first, own, peer, landed, peaks, landed_peaks, wide, total, mine, from_all,
    own_sem, rep_send, rep_recv, tile_send, tile_recv, peak_send, peak_recv,
    squares_send, squares_recv, state_sem, first_sem, met,
):
    rep, gx, gy = lax.axis_index("rep"), lax.axis_index("gx"), lax.axis_index("gy")
    steps, rows, cols = own.shape
    devices = replicas * rows_split * cols_split
    far = rows_split * (cols_split - 1)
    far_steps = far * matrices
    remote_steps = steps - matrices
    band = total.shape[0]
    spread, half = max(cols_split - 1, 1), cols_split // 2
    pieces = rows // band

    def band_at(index):
        return pl.ds(pl.multiple_of(index * band, band), band)

    def place(step, sign):
        turn, matrix = step // matrices, step % matrices
        is_far = turn < far
        row_shift = jnp.where(is_far, turn // spread, (turn - far + 1) % rows_split)
        col_shift = jnp.where(turn % spread < half, turn % spread, turn % spread + 1)
        col_shift = jnp.where(turn % spread == 0, half, col_shift)
        col_shift = jnp.where(is_far, col_shift, 0)
        c = (gx + rows_split + sign * row_shift) % rows_split
        d = (gy + cols_split + sign * col_shift) % cols_split
        return matrix, c, d

    def block(step, replica):
        matrix, c, d = place(step, 1)
        return delta_ref.at[matrix, c, replica, :, pl.ds(pl.multiple_of(d * cols, LANES), cols)]

    def own_copy(step):
        return pltpu.make_async_copy(block(step, rep), own.at[step], own_sem.at[step])

    def own_piece(piece):
        at = band_at(piece)
        return pltpu.make_async_copy(block(0, rep).at[at], own.at[0, at], own_sem.at[steps + piece])

    def first_piece(shift, piece):
        at = band_at(piece)
        target = (rep + shift) % replicas
        return pltpu.make_async_copy(block(0, target).at[at], first.at[shift - 1, at], first_sem.at[shift - 1, piece])

    def rep_piece(shift, piece):
        at = band_at(piece)
        target = (rep + shift) % replicas
        return pltpu.make_async_remote_copy(
            src_ref=first.at[shift - 1, at], dst_ref=peer.at[shift - 1, 0, at],
            send_sem=rep_send.at[shift - 1, steps + piece], recv_sem=rep_recv.at[shift - 1, steps + piece],
            device_id={"rep": target}, device_id_type=MESH,
        )

    def tile_pieces(piece):
        _, c, d = place(0, 1)
        at = band_at(piece)
        target = {"gx": c, "gy": d}
        return (
            pltpu.make_async_remote_copy(
                src_ref=own.at[0, at], dst_ref=landed.at[0, at],
                send_sem=tile_send.at[steps + piece], recv_sem=tile_recv.at[steps + piece],
                device_id=target, device_id_type=MESH,
            ),
            pltpu.make_async_remote_copy(
                src_ref=peaks.at[steps + piece], dst_ref=landed_peaks.at[steps + piece],
                send_sem=peak_send.at[steps + piece], recv_sem=peak_recv.at[steps + piece],
                device_id=target, device_id_type=MESH,
            ),
        )

    def rep_copy(shift, step):
        target = (rep + shift) % replicas
        return pltpu.make_async_remote_copy(
            src_ref=block(step, target), dst_ref=peer.at[shift - 1, step],
            send_sem=rep_send.at[shift - 1, step], recv_sem=rep_recv.at[shift - 1, step],
            device_id={"rep": target}, device_id_type=MESH,
        )

    def tile_copies(step):
        matrix, c, d = place(step, 1)
        target = {"gx": c, "gy": d}
        return (
            pltpu.make_async_remote_copy(
                src_ref=own.at[step], dst_ref=landed.at[step],
                send_sem=tile_send.at[step], recv_sem=tile_recv.at[step],
                device_id=target, device_id_type=MESH,
            ),
            pltpu.make_async_remote_copy(
                src_ref=peaks.at[step], dst_ref=landed_peaks.at[step],
                send_sem=peak_send.at[step], recv_sem=peak_recv.at[step],
                device_id=target, device_id_type=MESH,
            ),
        )

    def other(shift):
        place = ((gy * rows_split + gx) * replicas + rep + shift) % devices
        return {"gy": place // (rows_split * replicas), "gx": place // replicas % rows_split, "rep": place % replicas}

    def squares_copy(shift):
        return pltpu.make_async_remote_copy(
            src_ref=mine, dst_ref=from_all.at[shift - 1],
            send_sem=squares_send.at[shift - 1], recv_sem=squares_recv.at[shift - 1],
            device_id=other(shift), device_id_type=MESH,
        )

    def state_copies():
        return (
            pltpu.make_async_copy(params_ref, state_ref.at[pl.ds(steps, steps)], state_sem.at[0]),
            pltpu.make_async_copy(momentum_ref, state_ref.at[pl.ds(2 * steps, steps)], state_sem.at[1]),
        )

    def fetch_piece(piece, carry):
        for shift in range(1, replicas):
            first_piece(shift, piece).start()
        own_piece(piece).start()
        return carry

    lax.fori_loop(0, pieces, fetch_piece, 0)

    def greet_near(semaphore):
        for shift in range(1, rows_split):
            pl.semaphore_signal(
                semaphore, inc=1, device_id={"gx": (gx + shift) % rows_split}, device_id_type=MESH
            )

        @pl.when(gy > 0)
        def _():
            pl.semaphore_signal(semaphore, inc=1, device_id={"gy": gy - 1}, device_id_type=MESH)

        @pl.when(gy < cols_split - 1)
        def _():
            pl.semaphore_signal(semaphore, inc=1, device_id={"gy": gy + 1}, device_id_type=MESH)

    def greet_peers(semaphore):
        for shift in range(1, replicas):
            pl.semaphore_signal(
                semaphore, inc=1, device_id={"rep": (rep + shift) % replicas}, device_id_type=MESH
            )

    near = rows_split - 1 + (gy > 0).astype(jnp.int32) + (gy < cols_split - 1).astype(jnp.int32)
    barrier = pltpu.get_barrier_semaphore()
    greet_peers(barrier)
    greet_near(barrier)
    pl.semaphore_wait(barrier, replicas - 1 + near)

    def launch(step, carry):
        for shift in range(1, replicas):
            rep_copy(shift, step).start()
        return carry

    def launch_piece(piece, carry):
        for shift in range(1, replicas):
            first_piece(shift, piece).wait()
            rep_piece(shift, piece).start()
        return carry

    lax.fori_loop(0, pieces, launch_piece, 0)
    lax.fori_loop(1, steps, launch, 0)
    for relay in range(cols_split - 1):
        greet_near(met.at[relay])
        pl.semaphore_wait(met.at[relay], near)
    greet_peers(met.at[cols_split - 1])
    lax.fori_loop(1, steps, lambda step, carry: (own_copy(step).start(), carry)[1], 0)
    total[...] = jnp.zeros_like(total)

    def spot(matrix, c, d):
        return (matrix * rows_split + c) * cols_split + d

    def mean_of(step, at):
        value = own[step, at, :].astype(jnp.float32)
        for shift in range(1, replicas):
            value = value + peer[shift - 1, step, at, :].astype(jnp.float32)
        value = value * (1.0 / replicas)
        total[...] += value * value
        return value

    def arrive(step):
        own_copy(step).wait()
        for shift in range(1, replicas):
            rep_copy(shift, step).wait_recv()

    def unpack(step):
        for copy in tile_copies(step):
            copy.wait_recv()
        matrix, c, d = place(step, -1)
        lift = jnp.concatenate([landed_peaks[step]] * (cols // LANES), axis=1)

        def part(index, carry):
            at = band_at(index)
            state_ref[spot(matrix, c, d), at, :] = decode(landed[step, at, :]) * lift
            return carry

        lax.fori_loop(0, rows // band, part, 0)

    def unpack_pieces():
        matrix, c, d = place(0, -1)

        def part(piece, carry):
            for copy in tile_pieces(piece):
                copy.wait_recv()
            at = band_at(piece)
            lift = jnp.concatenate([landed_peaks[steps + piece]] * (cols // LANES), axis=1)
            state_ref[spot(matrix, c, d), at, :] = decode(landed[0, at, :]) * lift
            return carry

        lax.fori_loop(0, pieces, part, 0)

    def ready(step):
        return jnp.clip((3 * step - READY_LAG) // 4, 0, far_steps)

    def unpack_some(step):
        @pl.when((ready(step) > ready(step - 1)) & (ready(step) > 1))
        def _():
            unpack(ready(step) - 1)

        @pl.when(step >= far_steps + NEAR_LAG)
        def _():
            unpack(step - NEAR_LAG)

    def scales(peak):
        peak = jnp.maximum(jnp.max(peak, axis=0, keepdims=True), SMALLEST)
        return peak * (1.0 / TOP), jnp.concatenate([TOP / peak] * (cols // LANES), axis=1)

    def advance(step, carry):
        arrive(step)

        def average(index, peak):
            at = band_at(index)
            value = mean_of(step, at)
            wide[at, :] = value
            return jnp.maximum(peak, fold_lanes(jnp.abs(value), jnp.maximum))

        peak = lax.fori_loop(0, rows // band, average, jnp.zeros((band, LANES), jnp.float32))
        peaks[step], lift = scales(peak)

        def code(index, carry):
            at = band_at(index)
            own[step, at, :] = encode(wide[at, :] * lift)
            return carry

        lax.fori_loop(0, rows // band, code, 0)
        for copy in tile_copies(step):
            copy.start()

        @pl.when(step == PREFETCH_AT)
        def _():
            unpack_pieces()
            for copy in state_copies():
                copy.start()

        unpack_some(step)
        return carry

    def open_piece(piece, carry):
        own_piece(piece).wait()
        for shift in range(1, replicas):
            rep_piece(shift, piece).wait_recv()
        at = band_at(piece)
        value = mean_of(0, at)
        peaks[steps + piece], lift = scales(fold_lanes(jnp.abs(value), jnp.maximum))
        own[0, at, :] = encode(value * lift)
        for copy in tile_pieces(piece):
            copy.start()
        return carry

    lax.fori_loop(0, pieces, open_piece, 0)
    lax.fori_loop(1, remote_steps, advance, 0)

    def keep(step, carry):
        unpack_some(step)
        arrive(step)
        matrix = step - remote_steps

        def average(index, inner):
            at = band_at(index)
            state_ref[spot(matrix, gx, gy), at, :] = mean_of(step, at)
            return inner

        return lax.fori_loop(0, rows // band, average, carry)

    lax.fori_loop(remote_steps, steps, keep, 0)

    mine[...] = jnp.sum(fold_lanes(total[...], jnp.add), axis=0, keepdims=True)

    pl.semaphore_wait(met.at[cols_split - 1], replicas - 1)
    lax.fori_loop(1, devices, lambda shift, carry: (squares_copy(shift).start(), carry)[1], 0)

    last = ready(steps - 1)
    lax.fori_loop(last, far_steps, lambda step, carry: (unpack(step), carry)[1], 0)
    lax.fori_loop(
        max(steps - NEAR_LAG, far_steps), remote_steps, lambda step, carry: (unpack(step), carry)[1], 0
    )
    for copy in state_copies():
        copy.wait()

    def close_rep(step, carry):
        for shift in range(1, replicas):
            rep_copy(shift, step).wait_send()
        return carry

    def close_piece(piece, carry):
        for shift in range(1, replicas):
            rep_piece(shift, piece).wait_send()
        for copy in tile_pieces(piece):
            copy.wait_send()
        return carry

    lax.fori_loop(0, pieces, close_piece, 0)
    lax.fori_loop(1, steps, close_rep, 0)

    def close_send(step, carry):
        for copy in tile_copies(step):
            copy.wait_send()
        return carry

    lax.fori_loop(1, remote_steps, close_send, 0)

    def gather(shift, carry):
        squares_copy(shift).wait()
        return carry + from_all[shift - 1]

    state_ref[3 * steps, :1, :LANES] = lax.fori_loop(1, devices, gather, mine[...])


def update(entries, state_ref, new_params_ref, new_momentum_ref, params_out, momentum_out, sems):
    count, (rows, cols) = state_ref.shape[0] // 3, state_ref.shape[1:]
    squares = jnp.sum(state_ref[3 * count, :1, :LANES], axis=1, keepdims=True)
    clip_scale = jnp.minimum(1.0, clip_level / jnp.sqrt(squares / entries + epsilon))
    band = 8 if rows % 8 == 0 else rows

    def copies(tile):
        slot = tile % SLOTS
        return (
            pltpu.make_async_copy(params_out.at[slot], new_params_ref.at[tile], sems.at[0, slot]),
            pltpu.make_async_copy(momentum_out.at[slot], new_momentum_ref.at[tile], sems.at[1, slot]),
        )

    def one(tile, carry):
        slot = tile % SLOTS

        @pl.when(tile >= SLOTS)
        def _():
            for copy in copies(tile - SLOTS):
                copy.wait()

        def part(index, inner):
            at = pl.ds(pl.multiple_of(index * band, band), band)
            gradient = state_ref[tile, at, :] * clip_scale
            new_momentum = moment_decay * state_ref[2 * count + tile, at, :] + gradient
            momentum_out[slot, at, :] = new_momentum
            params_out[slot, at, :] = state_ref[count + tile, at, :] - outer_rate * (
                gradient + moment_decay * new_momentum
            )
            return inner

        lax.fori_loop(0, rows // band, part, 0, unroll=2 if (rows // band) % 2 == 0 else 1)
        for copy in copies(tile):
            copy.start()
        return carry

    lax.fori_loop(0, count, one, 0)

    def close(tile, carry):
        for copy in copies(tile):
            copy.wait()
        return carry

    lax.fori_loop(max(count - SLOTS, 0), count, close, 0)


def per_device(deltas, params, momentum):
    rows_split = lax.axis_size("gx")
    cols_split = lax.axis_size("gy")
    replicas = lax.axis_size("rep")
    matrices, local_rows, local_cols = deltas.shape[1:]
    rows = local_rows // (rows_split * replicas)
    cols = local_cols // cols_split
    entries = matrices * local_rows * local_cols * rows_split * cols_split
    grid = rows_split * cols_split
    devices = grid * replicas
    steps = grid * matrices
    band = 16 if rows % 16 == 0 else rows
    pieces = rows // band
    any_space = pl.BlockSpec(memory_space=pl.ANY)
    vmem = pl.BlockSpec(memory_space=pltpu.VMEM)
    dma = pltpu.SemaphoreType.DMA
    f32, bf16 = jnp.float32, jnp.bfloat16
    flat_shape = (steps, rows, cols)
    state = pl.pallas_call(
        functools.partial(exchange, replicas, rows_split, cols_split, matrices),
        out_shape=pltpu.VMEM((3 * steps + 1, rows, cols), f32),
        in_specs=[any_space] * 3,
        out_specs=vmem,
        scratch_shapes=[
            pltpu.VMEM((max(replicas - 1, 1), rows, cols), bf16),
            pltpu.VMEM(flat_shape, bf16),
            pltpu.VMEM((max(replicas - 1, 1), *flat_shape), bf16),
            pltpu.VMEM(flat_shape, bf16),
            pltpu.VMEM((steps + pieces, 1, LANES), f32),
            pltpu.VMEM((steps + pieces, 1, LANES), f32),
            pltpu.VMEM((rows, cols), f32),
            pltpu.VMEM((band, cols), f32),
            pltpu.VMEM((1, LANES), f32),
            pltpu.VMEM((devices, 1, LANES), f32),
            dma((steps + pieces,)),
            dma((max(replicas - 1, 1), steps + pieces)),
            dma((max(replicas - 1, 1), steps + pieces)),
            dma((steps + pieces,)),
            dma((steps + pieces,)),
            dma((steps + pieces,)),
            dma((steps + pieces,)),
            dma((devices,)),
            dma((devices,)),
            dma((2,)),
            dma((max(replicas - 1, 1), pieces)),
            pltpu.SemaphoreType.REGULAR((cols_split,)),
        ],
        compiler_params=pltpu.CompilerParams(
            collective_id=0, has_side_effects=True, vmem_limit_bytes=EXCHANGE_VMEM
        ),
    )(
        deltas.reshape(matrices, rows_split, replicas, rows, local_cols),
        params.reshape(flat_shape),
        momentum.reshape(flat_shape),
    )
    wide_shape = jax.ShapeDtypeStruct(flat_shape, f32)
    new_params, new_momentum = pl.pallas_call(
        functools.partial(update, entries),
        out_shape=(wide_shape, wide_shape),
        in_specs=[vmem],
        out_specs=(any_space, any_space),
        scratch_shapes=[
            pltpu.VMEM((min(SLOTS, steps), rows, cols), f32),
            pltpu.VMEM((min(SLOTS, steps), rows, cols), f32),
            dma((2, min(SLOTS, steps))),
        ],
        compiler_params=pltpu.CompilerParams(vmem_limit_bytes=UPDATE_VMEM),
    )(pltpu.with_memory_space_constraint(state, pltpu.VMEM))
    return (new_params.reshape(params.shape), new_momentum.reshape(momentum.shape))


def solution(mesh):
    placement = P(None, None, "gx", "rep", None, "gy", None, None)
    return jax.shard_map(
        per_device,
        mesh=mesh,
        in_specs=(P("rep", None, "gx", "gy"), placement, placement),
        out_specs=(placement, placement),
        check_vma=False,
    )
```

```python
import functools

import jax
import jax.numpy as jnp
from jax import lax
from jax.experimental import pallas as pl
from jax.experimental.pallas import tpu as pltpu
from jax.sharding import PartitionSpec as P

clip_level = 0.25
moment_decay = 0.9
outer_rate = 0.7
epsilon = 1e-06

MESH = pl.DeviceIdType.MESH
LANES = 128
TOP = 240.0
SMALLEST = 1e-30
SLOTS = 12
PREFETCH_AT = 4
READY_LAG = 21
NEAR_LAG = 5
EXCHANGE_VMEM = 22 * 1024 * 1024
UPDATE_VMEM = 20 * 1024 * 1024


def encode(value):
    power = value * value
    for _ in range(3):
        power = power * power
    return jnp.where(value < 0.0, -power, power).astype(jnp.bfloat16)


def decode(code):
    wide = code.astype(jnp.float32)
    root = jnp.exp2(jnp.log2(jnp.abs(wide)) * (1.0 / 16.0))
    root = jnp.where(wide == 0.0, 0.0, root)
    return jnp.where(wide < 0.0, -root, root)


def fold_lanes(tile, combine):
    folded = tile[:, :LANES]
    for start in range(LANES, tile.shape[1], LANES):
        folded = combine(folded, tile[:, start : start + LANES])
    return folded


def exchange(
    replicas, rows_split, cols_split, matrices,
    delta_ref, params_ref, momentum_ref, state_ref,
    first, own, peer, landed, peaks, landed_peaks, wide, total, mine, from_all,
    own_sem, rep_send, rep_recv, tile_send, tile_recv, peak_send, peak_recv,
    squares_send, squares_recv, state_sem, first_sem, met,
):
    rep, gx, gy = lax.axis_index("rep"), lax.axis_index("gx"), lax.axis_index("gy")
    steps, rows, cols = own.shape
    devices = replicas * rows_split * cols_split
    far = rows_split * (cols_split - 1)
    far_steps = far * matrices
    remote_steps = steps - matrices
    band = total.shape[0]
    group = rows_split * matrices
    spread, half = max(cols_split - 1, 1), cols_split // 2
    pieces = rows // band

    def band_at(index):
        return pl.ds(pl.multiple_of(index * band, band), band)

    def place(step, sign):
        turn, matrix = step // matrices, step % matrices
        is_far = turn < far
        row_shift = jnp.where(is_far, turn // spread, (turn - far + 1) % rows_split)
        col_shift = jnp.where(turn % spread < half, turn % spread, turn % spread + 1)
        col_shift = jnp.where(turn % spread == 0, half, col_shift)
        col_shift = jnp.where(is_far, col_shift, 0)
        c = (gx + rows_split + sign * row_shift) % rows_split
        d = (gy + cols_split + sign * col_shift) % cols_split
        return matrix, c, d

    def block(step, replica):
        matrix, c, d = place(step, 1)
        return delta_ref.at[matrix, c, replica, :, pl.ds(pl.multiple_of(d * cols, LANES), cols)]

    def own_copy(step):
        return pltpu.make_async_copy(block(step, rep), own.at[step], own_sem.at[step])

    def own_piece(piece):
        at = band_at(piece)
        return pltpu.make_async_copy(block(0, rep).at[at], own.at[0, at], own_sem.at[steps + piece])

    def first_piece(shift, piece):
        at = band_at(piece)
        target = (rep + shift) % replicas
        return pltpu.make_async_copy(block(0, target).at[at], first.at[shift - 1, at], first_sem.at[shift - 1, piece])

    def rep_piece(shift, piece):
        at = band_at(piece)
        target = (rep + shift) % replicas
        return pltpu.make_async_remote_copy(
            src_ref=first.at[shift - 1, at], dst_ref=peer.at[shift - 1, 0, at],
            send_sem=rep_send.at[shift - 1, steps + piece], recv_sem=rep_recv.at[shift - 1, steps + piece],
            device_id={"rep": target}, device_id_type=MESH,
        )

    def tile_pieces(piece):
        _, c, d = place(0, 1)
        at = band_at(piece)
        target = {"gx": c, "gy": d}
        return (
            pltpu.make_async_remote_copy(
                src_ref=own.at[0, at], dst_ref=landed.at[0, at],
                send_sem=tile_send.at[steps + piece], recv_sem=tile_recv.at[steps + piece],
                device_id=target, device_id_type=MESH,
            ),
            pltpu.make_async_remote_copy(
                src_ref=peaks.at[steps + piece], dst_ref=landed_peaks.at[steps + piece],
                send_sem=peak_send.at[steps + piece], recv_sem=peak_recv.at[steps + piece],
                device_id=target, device_id_type=MESH,
            ),
        )

    def rep_copy(shift, step):
        target = (rep + shift) % replicas
        return pltpu.make_async_remote_copy(
            src_ref=block(step, target), dst_ref=peer.at[shift - 1, step],
            send_sem=rep_send.at[shift - 1, step], recv_sem=rep_recv.at[shift - 1, step],
            device_id={"rep": target}, device_id_type=MESH,
        )

    def tile_copies(step):
        matrix, c, d = place(step, 1)
        target = {"gx": c, "gy": d}
        return (
            pltpu.make_async_remote_copy(
                src_ref=own.at[step], dst_ref=landed.at[step],
                send_sem=tile_send.at[step], recv_sem=tile_recv.at[step],
                device_id=target, device_id_type=MESH,
            ),
            pltpu.make_async_remote_copy(
                src_ref=peaks.at[step], dst_ref=landed_peaks.at[step],
                send_sem=peak_send.at[step], recv_sem=peak_recv.at[step],
                device_id=target, device_id_type=MESH,
            ),
        )

    def other(shift):
        place = ((gy * rows_split + gx) * replicas + rep + shift) % devices
        return {"gy": place // (rows_split * replicas), "gx": place // replicas % rows_split, "rep": place % replicas}

    def squares_copy(shift):
        return pltpu.make_async_remote_copy(
            src_ref=mine, dst_ref=from_all.at[shift - 1],
            send_sem=squares_send.at[shift - 1], recv_sem=squares_recv.at[shift - 1],
            device_id=other(shift), device_id_type=MESH,
        )

    def state_copies():
        return (
            pltpu.make_async_copy(params_ref, state_ref.at[pl.ds(steps, steps)], state_sem.at[0]),
            pltpu.make_async_copy(momentum_ref, state_ref.at[pl.ds(2 * steps, steps)], state_sem.at[1]),
        )

    def fetch_piece(piece, carry):
        for shift in range(1, replicas):
            first_piece(shift, piece).start()
        own_piece(piece).start()
        return carry

    lax.fori_loop(0, pieces, fetch_piece, 0)

    def greet_near(semaphore):
        for shift in range(1, rows_split):
            pl.semaphore_signal(
                semaphore, inc=1, device_id={"gx": (gx + shift) % rows_split}, device_id_type=MESH
            )

        @pl.when(gy > 0)
        def _():
            pl.semaphore_signal(semaphore, inc=1, device_id={"gy": gy - 1}, device_id_type=MESH)

        @pl.when(gy < cols_split - 1)
        def _():
            pl.semaphore_signal(semaphore, inc=1, device_id={"gy": gy + 1}, device_id_type=MESH)

    def greet_peers(semaphore):
        for shift in range(1, replicas):
            pl.semaphore_signal(
                semaphore, inc=1, device_id={"rep": (rep + shift) % replicas}, device_id_type=MESH
            )

    near = rows_split - 1 + (gy > 0).astype(jnp.int32) + (gy < cols_split - 1).astype(jnp.int32)
    barrier = pltpu.get_barrier_semaphore()
    greet_peers(barrier)
    greet_near(barrier)
    pl.semaphore_wait(barrier, replicas - 1 + near)

    def launch(step, carry):
        for shift in range(1, replicas):
            rep_copy(shift, step).start()
        return carry

    def launch_piece(piece, carry):
        for shift in range(1, replicas):
            first_piece(shift, piece).wait()
            rep_piece(shift, piece).start()
        return carry

    lax.fori_loop(0, pieces, launch_piece, 0)
    lax.fori_loop(1, steps, launch, 0)
    for relay in range(cols_split - 1):
        greet_near(met.at[relay])
        pl.semaphore_wait(met.at[relay], near)
    greet_peers(met.at[cols_split - 1])
    lax.fori_loop(1, steps, lambda step, carry: (own_copy(step).start(), carry)[1], 0)
    total[...] = jnp.zeros_like(total)

    def spot(matrix, c, d):
        return (matrix * rows_split + c) * cols_split + d

    def mean_of(step, at):
        value = own[step, at, :].astype(jnp.float32)
        for shift in range(1, replicas):
            value = value + peer[shift - 1, step, at, :].astype(jnp.float32)
        value = value * (1.0 / replicas)
        total[...] += value * value
        return value

    def arrive(step):
        own_copy(step).wait()
        for shift in range(1, replicas):
            rep_copy(shift, step).wait_recv()

    def unpack(step):
        for copy in tile_copies(step):
            copy.wait_recv()
        matrix, c, d = place(step, -1)
        lift = jnp.concatenate([landed_peaks[step]] * (cols // LANES), axis=1)

        def part(index, carry):
            at = band_at(index)
            state_ref[spot(matrix, c, d), at, :] = decode(landed[step, at, :]) * lift
            return carry

        lax.fori_loop(0, rows // band, part, 0)

    def unpack_pieces():
        matrix, c, d = place(0, -1)

        def part(piece, carry):
            for copy in tile_pieces(piece):
                copy.wait_recv()
            at = band_at(piece)
            lift = jnp.concatenate([landed_peaks[steps + piece]] * (cols // LANES), axis=1)
            state_ref[spot(matrix, c, d), at, :] = decode(landed[0, at, :]) * lift
            return carry

        lax.fori_loop(0, pieces, part, 0)

    def ready(step):
        return jnp.clip((3 * step - READY_LAG) // 4, 0, far_steps)

    def unpack_some(step):
        @pl.when((ready(step) > ready(step - 1)) & (ready(step) > 1))
        def _():
            unpack(ready(step) - 1)

        @pl.when(step >= far_steps + NEAR_LAG)
        def _():
            unpack(step - NEAR_LAG)

    def scales(peak):
        peak = jnp.maximum(jnp.max(peak, axis=0, keepdims=True), SMALLEST)
        return peak * (1.0 / TOP), jnp.concatenate([TOP / peak] * (cols // LANES), axis=1)

    def advance(step, carry):
        arrive(step)

        def average(index, peak):
            at = band_at(index)
            value = mean_of(step, at)
            wide[at, :] = value
            return jnp.maximum(peak, fold_lanes(jnp.abs(value), jnp.maximum))

        peak = lax.fori_loop(0, rows // band, average, jnp.zeros((band, LANES), jnp.float32))
        peaks[step], lift = scales(peak)

        def code(index, carry):
            at = band_at(index)
            own[step, at, :] = encode(wide[at, :] * lift)
            return carry

        lax.fori_loop(0, rows // band, code, 0)
        for copy in tile_copies(step):
            copy.start()

        @pl.when(step == PREFETCH_AT)
        def _():
            unpack_pieces()
            for copy in state_copies():
                copy.start()

        unpack_some(step)
        return carry

    def open_piece(piece, carry):
        own_piece(piece).wait()
        for shift in range(1, replicas):
            rep_piece(shift, piece).wait_recv()
        at = band_at(piece)
        value = mean_of(0, at)
        peaks[steps + piece], lift = scales(fold_lanes(jnp.abs(value), jnp.maximum))
        own[0, at, :] = encode(value * lift)
        for copy in tile_pieces(piece):
            copy.start()
        return carry

    lax.fori_loop(0, pieces, open_piece, 0)
    lax.fori_loop(1, remote_steps, advance, 0)

    def keep(step, carry):
        unpack_some(step)
        arrive(step)
        matrix = step - remote_steps

        def average(index, inner):
            at = band_at(index)
            state_ref[spot(matrix, gx, gy), at, :] = mean_of(step, at)
            return inner

        return lax.fori_loop(0, rows // band, average, carry)

    lax.fori_loop(remote_steps, steps, keep, 0)

    mine[...] = jnp.sum(fold_lanes(total[...], jnp.add), axis=0, keepdims=True)

    pl.semaphore_wait(met.at[cols_split - 1], replicas - 1)
    lax.fori_loop(1, devices, lambda shift, carry: (squares_copy(shift).start(), carry)[1], 0)

    early = max(far_steps - group, 1)
    def close_rep(step, carry):
        for shift in range(1, replicas):
            rep_copy(shift, step).wait_send()
        return carry

    def close_piece(piece, carry):
        for shift in range(1, replicas):
            rep_piece(shift, piece).wait_send()
        for copy in tile_pieces(piece):
            copy.wait_send()
        return carry

    lax.fori_loop(0, pieces, close_piece, 0)
    lax.fori_loop(1, steps, close_rep, 0)

    def close_send(step, carry):
        for copy in tile_copies(step):
            copy.wait_send()
        return carry

    lax.fori_loop(1, early, close_send, 0)

    last = ready(steps - 1)
    lax.fori_loop(
        max(steps - NEAR_LAG, far_steps), remote_steps, lambda step, carry: (unpack(step), carry)[1], 0
    )
    lax.fori_loop(last, far_steps, lambda step, carry: (unpack(step), carry)[1], 0)
    for copy in state_copies():
        copy.wait()

    lax.fori_loop(early, remote_steps, close_send, 0)

    def gather(shift, carry):
        squares_copy(shift).wait()
        return carry + from_all[shift - 1]

    state_ref[3 * steps, :1, :LANES] = lax.fori_loop(1, devices, gather, mine[...])


def update(entries, state_ref, new_params_ref, new_momentum_ref, params_out, momentum_out, sems):
    count, (rows, cols) = state_ref.shape[0] // 3, state_ref.shape[1:]
    squares = jnp.sum(state_ref[3 * count, :1, :LANES], axis=1, keepdims=True)
    clip_scale = jnp.minimum(1.0, clip_level / jnp.sqrt(squares / entries + epsilon))
    band = 8 if rows % 8 == 0 else rows

    def copies(tile):
        slot = tile % SLOTS
        return (
            pltpu.make_async_copy(params_out.at[slot], new_params_ref.at[tile], sems.at[0, slot]),
            pltpu.make_async_copy(momentum_out.at[slot], new_momentum_ref.at[tile], sems.at[1, slot]),
        )

    def one(tile, carry):
        slot = tile % SLOTS

        @pl.when(tile >= SLOTS)
        def _():
            for copy in copies(tile - SLOTS):
                copy.wait()

        def part(index, inner):
            at = pl.ds(pl.multiple_of(index * band, band), band)
            gradient = state_ref[tile, at, :] * clip_scale
            new_momentum = moment_decay * state_ref[2 * count + tile, at, :] + gradient
            momentum_out[slot, at, :] = new_momentum
            params_out[slot, at, :] = state_ref[count + tile, at, :] - outer_rate * (
                gradient + moment_decay * new_momentum
            )
            return inner

        lax.fori_loop(0, rows // band, part, 0, unroll=2 if (rows // band) % 2 == 0 else 1)
        for copy in copies(tile):
            copy.start()
        return carry

    lax.fori_loop(0, count, one, 0)

    def close(tile, carry):
        for copy in copies(tile):
            copy.wait()
        return carry

    lax.fori_loop(max(count - SLOTS, 0), count, close, 0)


def per_device(deltas, params, momentum):
    rows_split = lax.axis_size("gx")
    cols_split = lax.axis_size("gy")
    replicas = lax.axis_size("rep")
    matrices, local_rows, local_cols = deltas.shape[1:]
    rows = local_rows // (rows_split * replicas)
    cols = local_cols // cols_split
    entries = matrices * local_rows * local_cols * rows_split * cols_split
    grid = rows_split * cols_split
    devices = grid * replicas
    steps = grid * matrices
    band = 16 if rows % 16 == 0 else rows
    pieces = rows // band
    any_space = pl.BlockSpec(memory_space=pl.ANY)
    vmem = pl.BlockSpec(memory_space=pltpu.VMEM)
    dma = pltpu.SemaphoreType.DMA
    f32, bf16 = jnp.float32, jnp.bfloat16
    flat_shape = (steps, rows, cols)
    state = pl.pallas_call(
        functools.partial(exchange, replicas, rows_split, cols_split, matrices),
        out_shape=pltpu.VMEM((3 * steps + 1, rows, cols), f32),
        in_specs=[any_space] * 3,
        out_specs=vmem,
        scratch_shapes=[
            pltpu.VMEM((max(replicas - 1, 1), rows, cols), bf16),
            pltpu.VMEM(flat_shape, bf16),
            pltpu.VMEM((max(replicas - 1, 1), *flat_shape), bf16),
            pltpu.VMEM(flat_shape, bf16),
            pltpu.VMEM((steps + pieces, 1, LANES), f32),
            pltpu.VMEM((steps + pieces, 1, LANES), f32),
            pltpu.VMEM((rows, cols), f32),
            pltpu.VMEM((band, cols), f32),
            pltpu.VMEM((1, LANES), f32),
            pltpu.VMEM((devices, 1, LANES), f32),
            dma((steps + pieces,)),
            dma((max(replicas - 1, 1), steps + pieces)),
            dma((max(replicas - 1, 1), steps + pieces)),
            dma((steps + pieces,)),
            dma((steps + pieces,)),
            dma((steps + pieces,)),
            dma((steps + pieces,)),
            dma((devices,)),
            dma((devices,)),
            dma((2,)),
            dma((max(replicas - 1, 1), pieces)),
            pltpu.SemaphoreType.REGULAR((cols_split,)),
        ],
        compiler_params=pltpu.CompilerParams(
            collective_id=0, has_side_effects=True, vmem_limit_bytes=EXCHANGE_VMEM
        ),
    )(
        deltas.reshape(matrices, rows_split, replicas, rows, local_cols),
        params.reshape(flat_shape),
        momentum.reshape(flat_shape),
    )
    wide_shape = jax.ShapeDtypeStruct(flat_shape, f32)
    new_params, new_momentum = pl.pallas_call(
        functools.partial(update, entries),
        out_shape=(wide_shape, wide_shape),
        in_specs=[vmem],
        out_specs=(any_space, any_space),
        scratch_shapes=[
            pltpu.VMEM((min(SLOTS, steps), rows, cols), f32),
            pltpu.VMEM((min(SLOTS, steps), rows, cols), f32),
            dma((2, min(SLOTS, steps))),
        ],
        compiler_params=pltpu.CompilerParams(vmem_limit_bytes=UPDATE_VMEM),
    )(pltpu.with_memory_space_constraint(state, pltpu.VMEM))
    return (new_params.reshape(params.shape), new_momentum.reshape(momentum.shape))


def solution(mesh):
    placement = P(None, None, "gx", "rep", None, "gy", None, None)
    return jax.shard_map(
        per_device,
        mesh=mesh,
        in_specs=(P("rep", None, "gx", "gy"), placement, placement),
        out_specs=(placement, placement),
        check_vma=False,
    )
```
